32 devices in a mesh: blk: 8 (over z, x), tgt: 4 (over y, core).
Axes of the slice: x: 2, y: 2, z: 4, core: 2. Of those that a mesh axis runs over, the one named last changes fastest.
Arguments:
- sources: float32 [8192, 128], P('blk'), may hold values from -0.5 to 0.5, as said below
- targets: float32 [8192, 128], P(('blk', 'tgt')), may hold values from -0.5 to 0.5, as said below
- duals_init: float32 [8192], P(('blk', 'tgt')), may hold values from -1.5 to 1.5
Outputs:
- source_duals: float32 [8192], P('blk')
- target_duals: float32 [8192], P(('blk', 'tgt'))
The draws below stay inside these ranges and needn't reach their ends.
Inputs may be any that keep to these rules, and one draw needn't show every extreme that they name: `sources`: coordinates of the source points. `targets`: coordinates of the target points.
All inputs are finite; a program needn't handle non-finite values.
Results may differ from the reference program's by a relative error of at most 0.0001.
Values sent between devices are 32-bit elements; how exact they have to be, the bound alone decides.
A program may use at most 64 MiB of HBM per device.

```python
import jax
import jax.numpy as jnp
from jax import lax

D = 128
ROWS_DEV = 1024
TGT_DEV = 256
ITERS = 2
N_SRC = 8192
N_DST = 8192


def common_offset(key):
    inner = jax.random.fold_in(key, 11)
    size_key, sign_key = jax.random.split(inner)
    magnitude = jax.random.uniform(size_key, (D,), jnp.float32, 0.15, 0.25)
    signs = jnp.where(jax.random.bernoulli(sign_key, 0.5, (D,)), 1.0, -1.0)
    return magnitude * signs


def cloud_points(key, salt, count):
    offset = common_offset(key)
    inner = jax.random.fold_in(key, salt)
    base_key, pick_key, sign_key, size_key = jax.random.split(inner, 4)
    base = 0.0625 * jax.random.truncated_normal(base_key, -6.0, 6.0, (count, D), jnp.float32)
    chosen = jax.random.randint(pick_key, (count,), 0, 48) == 0
    signs = jnp.where(jax.random.bernoulli(sign_key, 0.5, (count, D)), 1.0, -1.0)
    strength = jax.random.uniform(size_key, (count, 1), jnp.float32, 0.6, 1.0)
    far_part = 0.45 * strength * signs
    local = jnp.where(chosen[:, None], far_part, base)
    return jnp.clip(offset[None, :] + local, -0.5, 0.5)


def draw_sources(key, part):
    return cloud_points(key, 3, N_SRC)


def draw_targets(key, part):
    return cloud_points(key, 5, N_DST)


def steps_of(stream_key, shape, cuts, smallest, high):
    loudness, own = 1.0, jax.random.fold_in(stream_key, 6)
    for dim, shards_of in cuts:
        draws = jnp.exp(jax.random.uniform(jax.random.fold_in(own, dim), (shards_of,), jnp.float32, smallest / len(cuts), high / len(cuts)))
        loudness = loudness * jnp.repeat(draws, shape[dim] // shards_of).reshape([-1 if axis == dim else 1 for axis in range(len(shape))])
    return loudness


def scatter_about(own_key, extent, deviation, bound, pieces=(), held_as=jnp.bfloat16):
    entries = deviation * jax.random.normal(own_key, extent, jnp.float32)
    if pieces:
        entries = entries * steps_of(own_key, extent, pieces, -0.22, 0.18)
    return jnp.clip(entries, -bound, bound).astype(held_as)


def setup_inputs(seed: int = 0) -> dict:
    arg_keys = jax.random.split(jax.random.key(seed), 4)
    sources = draw_sources(jax.random.fold_in(arg_keys[3], 71), 0)
    targets = draw_targets(jax.random.fold_in(arg_keys[3], 71), 0)
    duals_init = scatter_about(arg_keys[2], (N_DST,), 0.3, 1.5, ((0, 32),), jnp.float32)
    return {"sources": sources, "targets": targets, "duals_init": duals_init}


EPS = 0.05


def block_lse(left_blk, left_norm, right, right_norm, right_pots):
    cross = jnp.dot(left_blk, right.T, preferred_element_type=jnp.float32, precision=lax.Precision.HIGHEST)
    cost_tile = left_norm[:, None] + right_norm[None, :] - 2.0 * cross
    scores = (right_pots[None, :] - cost_tile) / EPS
    maxima = jnp.max(scores, axis=1)
    return maxima + jnp.log(jnp.sum(jnp.exp(scores - maxima[:, None]), axis=1))


def half_step(left, left_norm, right, right_norm, right_pots, block):
    count = left.shape[0] // block
    left_blocks = left.reshape(count, block, left.shape[1])
    norm_blocks = left_norm.reshape(count, block)
    result = lax.map(lambda pair: block_lse(pair[0], pair[1], right, right_norm, right_pots), (left_blocks, norm_blocks))
    return EPS * (-jnp.log(jnp.float32(right.shape[0]))) - EPS * result.reshape(-1)


def reference(sources, targets, duals_init):
    src_norm = jnp.sum(sources * sources, axis=1)
    dst_norm = jnp.sum(targets * targets, axis=1)
    target_pots = duals_init
    source_pots = jnp.zeros_like(src_norm)
    for repeat in range(ITERS):
        source_pots = half_step(sources, src_norm, targets, dst_norm, target_pots, ROWS_DEV)
        target_pots = half_step(targets, dst_norm, sources, src_norm, source_pots, TGT_DEV)
    return source_pots, target_pots
```

```python
import functools
import math

import jax
import jax.numpy as jnp
from jax import lax
from jax.experimental import pallas as pl
from jax.experimental.pallas import tpu as pltpu
from jax.sharding import PartitionSpec as P

ITERS = 2
EPS = 0.05
LOG2E = math.log2(math.e)
SCALE = LOG2E / EPS
MESH = pl.DeviceIdType.MESH
LANES = 128
COLS_CHUNK_ROWS = 32
DOT_ROWS = 128


def log2_of(value):
    return jnp.log(value) * LOG2E


def pieces_of(value, count):
    parts = []
    for _ in range(count):
        part = value.astype(jnp.bfloat16)
        parts.append(part)
        value = value - part.astype(jnp.float32)
    return parts


def extended(points, scale, norm_first):
    norm = -SCALE * jnp.sum(points * points, axis=1, keepdims=True)
    hi, lo = pieces_of(points * scale, 2)
    first, second, third = (part.astype(jnp.float32) for part in pieces_of(norm, 3))
    lane = lax.broadcasted_iota(jnp.int32, points.shape, 1)
    base = 0 if norm_first else 3
    ones = 3 - base
    extra = jnp.where((lane >= ones) & (lane < ones + 3), 1.0, 0.0)
    extra = jnp.where(lane == base, first, extra)
    extra = jnp.where(lane == base + 1, second, extra)
    extra = jnp.where(lane == base + 2, third, extra)
    middle = (lo, hi) if norm_first else (hi, lo)
    return jnp.concatenate([hi, middle[0], middle[1], extra.astype(jnp.bfloat16)], axis=1)


def kernel(
    n_hi, n_th, src_ref, tgt_ref, dual_ref, src_out, tgt_out,
    src_in, left, right, cost, blocks, duals, top, acc, shift, pots, row_buf, col_buf, fin_mine, fin_buf, out_mine, out_buf,
    s_sem, z_send, z_recv, zd_send, zd_recv, f_send, f_recv, fd_send, fd_recv, r_send, r_recv, c_send, c_recv, o_sem,
):
    rows, width = src_ref.shape
    own = tgt_ref.shape[0]
    pair = 2 * own
    n_src = rows * n_hi * 2
    n_dst = own * n_hi * 2 * n_th * 2
    b, t = lax.axis_index("blk"), lax.axis_index("tgt")
    hi, lo = lax.div(b, 2), lax.rem(b, 2)
    th, tl = lax.div(t, 2), lax.rem(t, 2)

    def col_peer(dh, dl):
        return (lax.rem(hi + dh, n_hi) * 2 + lo, th * 2 + lax.rem(tl + dl, 2))

    def row_peer(dlo, dth):
        return (hi * 2 + lax.rem(lo + dlo, 2), lax.rem(th + dth, n_th) * 2 + tl)

    col_moves = [(dh, dl) for dh in range(n_hi) for dl in range(2) if dh or dl]
    row_moves = [(dlo, dth) for dlo in range(2) for dth in range(n_th) if dlo or dth]
    my_col = hi * 2 + tl
    my_row = lo * n_th + th

    def remote(src, dst, send, recv, peer):
        return pltpu.make_async_remote_copy(
            src_ref=src, dst_ref=dst, send_sem=send, recv_sem=recv, device_id=peer, device_id_type=MESH
        )

    barrier = pltpu.get_barrier_semaphore()
    peers = [col_peer(*move) for move in col_moves] + [row_peer(*move) for move in row_moves]
    for peer in peers:
        pl.semaphore_signal(barrier, inc=1, device_id=peer, device_id_type=MESH)

    def fill_left(ref):
        def step(index, carry):
            at = pl.ds(pl.multiple_of(index * LANES, LANES), LANES)
            left[at, :] = extended(ref[at, :], 1.0, True)
            return carry

        lax.fori_loop(0, rows // LANES, step, 0)

    pl.semaphore_wait(barrier, len(peers))

    has_rows = lo == tl
    swap = remote(src_ref, src_in, s_sem.at[0], s_sem.at[1], row_peer(1, 0))

    started = []
    z_copies, f_copies = {}, {}
    for dh in range(1, n_hi):
        z_copies[dh] = (
            remote(dual_ref, duals.at[hi, tl], zd_send.at[dh], zd_recv.at[dh], col_peer(dh, 0)),
            remote(tgt_ref, blocks.at[hi, tl], z_send.at[dh], z_recv.at[dh], col_peer(dh, 0)),
        )
        for copy in z_copies[dh]:
            copy.start()

    @pl.when(has_rows)
    def _():
        swap.start()

    f_copies[0] = (
        remote(dual_ref, duals.at[hi, tl], fd_send.at[0], fd_recv.at[0], col_peer(0, 1)),
        remote(tgt_ref, blocks.at[hi, tl], f_send.at[0], f_recv.at[0], col_peer(0, 1)),
    )
    for copy in f_copies[0]:
        copy.start()
    blocks[hi, tl] = tgt_ref[...]
    duals[hi, tl] = dual_ref[...]

    @pl.when(has_rows)
    def _():
        fill_left(src_ref)

    @pl.when(jnp.logical_not(has_rows))
    def _():
        swap.wait_recv()
        fill_left(src_in)

    def use_pair(h, first):
        for c in range(2):
            right[c * own : (c + 1) * own, :] = extended(blocks[h, c], 2.0 * SCALE, False)
        pots_here = SCALE * jnp.concatenate([duals[h, 0], duals[h, 1]], axis=1)

        def step(index, carry):
            at = pl.ds(pl.multiple_of(index * DOT_ROWS, DOT_ROWS), DOT_ROWS)
            tile = lax.dot_general(
                left[at, :], right[...], (((1,), (1,)), ((), ())), preferred_element_type=jnp.float32
            )
            cost[h, at, :] = tile
            scores = [
                tile[:, k : k + LANES] + pots_here[:, k : k + LANES] for k in range(0, pair, LANES)
            ]
            high = functools.reduce(jnp.maximum, scores)
            if not first:
                before = top[at, :]
                high = jnp.maximum(high, before)
            total = sum(jnp.exp2(score - high) for score in scores)
            if not first:
                total = total + acc[at, :] * jnp.exp2(before - high)
            top[at, :] = high
            acc[at, :] = total
            return carry

        lax.fori_loop(0, rows // DOT_ROWS, step, 0)

    for dh in range(n_hi):
        h = lax.rem(hi + n_hi - dh, n_hi)
        if dh:
            for copy in z_copies[dh]:
                copy.wait_recv()
            f_copies[dh] = (
                remote(duals.at[h, tl], duals.at[h, tl], fd_send.at[dh], fd_recv.at[dh], col_peer(0, 1)),
                remote(blocks.at[h, tl], blocks.at[h, tl], f_send.at[dh], f_recv.at[dh], col_peer(0, 1)),
            )
            for copy in f_copies[dh]:
                copy.start()
        for copy in f_copies[dh]:
            copy.wait_recv()
        use_pair(h, dh == 0)

    def row_pass():
        def step(index, carry):
            at = pl.ds(pl.multiple_of(index * 8, 8), 8)
            scores = [
                cost[h, at, k : k + LANES] + pots[h : h + 1, k : k + LANES]
                for h in range(n_hi)
                for k in range(0, pair, LANES)
            ]
            high = functools.reduce(jnp.maximum, scores)
            top[at, :] = high
            acc[at, :] = sum(jnp.exp2(score - high) for score in scores)
            return carry

        lax.fori_loop(0, rows // 8, step, 0, unroll=2)

    def col_pass(h):
        groups = COLS_CHUNK_ROWS // 8

        def step(index, carry):
            high, total = carry
            at = pl.ds(pl.multiple_of(index * COLS_CHUNK_ROWS, COLS_CHUNK_ROWS), COLS_CHUNK_ROWS)
            offs = shift[at, :]
            new_high, new_total = [], []
            tile = cost[h, at, :]
            for k in range(pair // LANES):
                scores = tile[:, k * LANES : (k + 1) * LANES] + offs
                parts = [scores[g * 8 : (g + 1) * 8] for g in range(groups)]
                best = jnp.maximum(high[k], functools.reduce(jnp.maximum, parts))
                part = sum(jnp.exp2(value - best) for value in parts)
                new_total.append(total[k] * jnp.exp2(high[k] - best) + part)
                new_high.append(best)
            return tuple(new_high), tuple(new_total)

        lowest = tuple(jnp.full((8, LANES), -1e38, jnp.float32) for _ in range(pair // LANES))
        zero = tuple(jnp.zeros((8, LANES), jnp.float32) for _ in range(pair // LANES))
        high, total = lax.fori_loop(0, rows // COLS_CHUNK_ROWS, step, (lowest, zero), unroll=2)
        high, total = jnp.concatenate(high, axis=1), jnp.concatenate(total, axis=1)
        best = jnp.max(high, axis=0, keepdims=True)
        return best + log2_of(jnp.sum(total * jnp.exp2(high - best), axis=0, keepdims=True))

    def joined(values):
        best = functools.reduce(jnp.maximum, values)
        return best + log2_of(sum(jnp.exp2(value - best) for value in values))

    pending = []
    for turn in range(ITERS):
        last = turn == ITERS - 1
        if turn:
            row_pass()
        for k in range(rows // LANES):
            high = top[k * LANES : (k + 1) * LANES, :].T
            total = acc[k * LANES : (k + 1) * LANES, :].T
            best = jnp.max(high, axis=0, keepdims=True)
            total = jnp.sum(total * jnp.exp2(high - best), axis=0, keepdims=True)
            row_buf[turn, my_row, k : k + 1, :] = best + log2_of(total)
        copies = []
        for index, move in enumerate(row_moves):
            mine = row_buf.at[turn, my_row]
            copies.append(remote(mine, mine, r_send.at[turn, index], r_recv.at[turn, index], row_peer(*move)))
            copies[-1].start()
        for copy in copies:
            copy.wait_recv()
        pending += copies
        offs = -math.log2(n_dst) - joined([row_buf[turn, g] for g in range(2 * n_th)])
        if last:
            out_mine[...] = offs * (1.0 / SCALE)
            hand = remote(out_mine, out_buf, o_sem.at[0], o_sem.at[1], col_peer(0, 1))

            @pl.when(has_rows)
            def _():
                hand.start()

        for k in range(rows // LANES):
            spread = jnp.broadcast_to(offs[k : k + 1, :], (LANES, LANES))
            shift[k * LANES : (k + 1) * LANES, :] = spread.T
        if not last:
            for h in range(n_hi):
                col_buf[turn, my_col, h : h + 1, :] = col_pass(h)
            copies = []
            for index, move in enumerate(col_moves):
                mine = col_buf.at[turn, my_col]
                copies.append(remote(mine, mine, c_send.at[turn, index], c_recv.at[turn, index], col_peer(*move)))
                copies[-1].start()
            for copy in copies:
                copy.wait_recv()
            pending += copies
            pots[...] = -math.log2(n_src) - joined([col_buf[turn, g] for g in range(2 * n_hi)])
        else:
            for h in range(n_hi):
                value = col_pass(h)
                for c in range(2):
                    fin_mine[h, c] = value[:, c * own : (c + 1) * own]
            copies = []
            for index, (dh, dl) in enumerate(col_moves):
                mine = fin_mine.at[lax.rem(hi + dh, n_hi), lax.rem(tl + dl, 2)]
                copies.append(
                    remote(mine, fin_buf.at[my_col], c_send.at[turn, index], c_recv.at[turn, index], col_peer(dh, dl))
                )
                copies[-1].start()
            fin_buf[my_col] = fin_mine[hi, tl]
            for copy in copies:
                copy.wait_recv()
            pending += copies
            value = -math.log2(n_src) - joined([fin_buf[g] for g in range(2 * n_hi)])
            tgt_out[...] = value * (1.0 / SCALE)

    @pl.when(has_rows)
    def _():
        src_out[...] = out_mine[...]
        hand.wait_send()
        swap.wait_send()

    @pl.when(jnp.logical_not(has_rows))
    def _():
        hand.wait_recv()
        src_out[...] = out_buf[...]

    for group in list(z_copies.values()) + list(f_copies.values()):
        for copy in group:
            copy.wait_send()
    for copy in pending:
        copy.wait_send()


def body(sources, targets, duals_init, n_hi, n_th):
    rows, width = sources.shape
    own = targets.shape[0]
    pair = 2 * own
    vmem = pl.BlockSpec(memory_space=pltpu.VMEM)
    dma = pltpu.SemaphoreType.DMA
    f32 = jnp.float32
    source_pots, target_pots = pl.pallas_call(
        functools.partial(kernel, n_hi, n_th),
        out_shape=(
            jax.ShapeDtypeStruct((rows // LANES, LANES), f32),
            jax.ShapeDtypeStruct((1, own), f32),
        ),
        in_specs=[vmem] * 3,
        out_specs=(vmem, vmem),
        scratch_shapes=[
            pltpu.VMEM((rows, width), f32),
            pltpu.VMEM((rows, 4 * width), jnp.bfloat16),
            pltpu.VMEM((pair, 4 * width), jnp.bfloat16),
            pltpu.VMEM((n_hi, rows, pair), f32),
            pltpu.VMEM((n_hi, 2, own, width), f32),
            pltpu.VMEM((n_hi, 2, 1, own), f32),
            pltpu.VMEM((rows, LANES), f32),
            pltpu.VMEM((rows, LANES), f32),
            pltpu.VMEM((rows, LANES), f32),
            pltpu.VMEM((n_hi, pair), f32),
            pltpu.VMEM((ITERS, 2 * n_th, rows // LANES, LANES), f32),
            pltpu.VMEM((ITERS, 2 * n_hi, n_hi, pair), f32),
            pltpu.VMEM((n_hi, 2, 1, own), f32),
            pltpu.VMEM((2 * n_hi, 1, own), f32),
            pltpu.VMEM((rows // LANES, LANES), f32),
            pltpu.VMEM((rows // LANES, LANES), f32),
            dma((2,)),
            dma((n_hi,)), dma((n_hi,)), dma((n_hi,)), dma((n_hi,)),
            dma((n_hi,)), dma((n_hi,)), dma((n_hi,)), dma((n_hi,)),
            dma((ITERS, 2 * n_th)), dma((ITERS, 2 * n_th)),
            dma((ITERS, 2 * n_hi)), dma((ITERS, 2 * n_hi)),
            dma((2,)),
        ],
        compiler_params=pltpu.CompilerParams(
            collective_id=0, has_side_effects=True, vmem_limit_bytes=60 * 1024 * 1024
        ),
    )(sources, targets, duals_init.reshape(1, own))
    return source_pots.reshape(rows), target_pots.reshape(own)


def solution(mesh):
    n_hi, n_th = mesh.shape["blk"] // 2, mesh.shape["tgt"] // 2
    return jax.shard_map(
        functools.partial(body, n_hi=n_hi, n_th=n_th),
        mesh=mesh,
        in_specs=(P("blk", None), P(("blk", "tgt"), None), P(("blk", "tgt"))),
        out_specs=(P("blk"), P(("blk", "tgt"))),
        check_vma=False,
    )
```

```python
import functools
import math

import jax
import jax.numpy as jnp
from jax import lax
from jax.experimental import pallas as pl
from jax.experimental.pallas import tpu as pltpu
from jax.sharding import PartitionSpec as P

ITERS = 2
EPS = 0.05
LOG2E = math.log2(math.e)
SCALE = LOG2E / EPS
MESH = pl.DeviceIdType.MESH
LANES = 128
COLS_CHUNK_ROWS = 32
DOT_ROWS = 512
SWAPS = 4


def log2_of(value):
    return jnp.log(value) * LOG2E


def pieces_of(value, count):
    parts = []
    for _ in range(count):
        part = value.astype(jnp.bfloat16)
        parts.append(part)
        value = value - part.astype(jnp.float32)
    return parts


def extended(points, scale, norm_first):
    norm = -SCALE * jnp.sum(points * points, axis=1, keepdims=True)
    hi, lo = pieces_of(points * scale, 2)
    first, second, third = (part.astype(jnp.float32) for part in pieces_of(norm, 3))
    lane = lax.broadcasted_iota(jnp.int32, points.shape, 1)
    base = 0 if norm_first else 3
    ones = 3 - base
    extra = jnp.where((lane >= ones) & (lane < ones + 3), 1.0, 0.0)
    extra = jnp.where(lane == base, first, extra)
    extra = jnp.where(lane == base + 1, second, extra)
    extra = jnp.where(lane == base + 2, third, extra)
    middle = (lo, hi) if norm_first else (hi, lo)
    return jnp.concatenate([hi, middle[0], middle[1], extra.astype(jnp.bfloat16)], axis=1)


def kernel(
    n_hi, n_th, src_ref, tgt_ref, dual_ref, src_out, tgt_out,
    src_in, left, right, cost, blocks, duals, top, acc, shift, pots, row_buf, col_buf, fin_mine, fin_buf, out_mine, out_buf,
    s_send, s_recv, z_send, z_recv, zd_send, zd_recv, f_send, f_recv, fd_send, fd_recv, r_send, r_recv, c_send, c_recv, o_sem,
):
    rows, width = src_ref.shape
    own = tgt_ref.shape[0]
    pair = 2 * own
    n_src = rows * n_hi * 2
    n_dst = own * n_hi * 2 * n_th * 2
    b, t = lax.axis_index("blk"), lax.axis_index("tgt")
    hi, lo = lax.div(b, 2), lax.rem(b, 2)
    th, tl = lax.div(t, 2), lax.rem(t, 2)

    def col_peer(dh, dl):
        return (lax.rem(hi + dh, n_hi) * 2 + lo, th * 2 + lax.rem(tl + dl, 2))

    def row_peer(dlo, dth):
        return (hi * 2 + lax.rem(lo + dlo, 2), lax.rem(th + dth, n_th) * 2 + tl)

    col_moves = [(dh, dl) for dh in range(n_hi) for dl in range(2) if dh or dl]
    row_moves = [(dlo, dth) for dlo in range(2) for dth in range(n_th) if dlo or dth]
    my_col = hi * 2 + tl
    my_row = lo * n_th + th

    def remote(src, dst, send, recv, peer):
        return pltpu.make_async_remote_copy(
            src_ref=src, dst_ref=dst, send_sem=send, recv_sem=recv, device_id=peer, device_id_type=MESH
        )

    barrier = pltpu.get_barrier_semaphore()
    peers = [col_peer(*move) for move in col_moves] + [row_peer(*move) for move in row_moves]
    for peer in peers:
        pl.semaphore_signal(barrier, inc=1, device_id=peer, device_id_type=MESH)

    ordered = [jnp.int32(0)] * (n_hi - 1)
    found = jnp.int32(0)
    for distance in range(1, n_hi):
        for place in (hi - distance, hi + distance):
            valid = jnp.where((place >= 0) & (place < n_hi), 1, 0)
            for k in range(n_hi - 1):
                ordered[k] = ordered[k] + jnp.where(found == k, 1, 0) * valid * place
            found = found + valid

    def z_peer(place):
        return (place * 2 + lo, t)

    piece = rows // SWAPS

    def fill_left(ref, part):
        def step(index, carry):
            at = pl.ds(pl.multiple_of(part * piece + index * LANES, LANES), LANES)
            left[at, :] = extended(ref[at, :], 1.0, True)
            return carry

        lax.fori_loop(0, piece // LANES, step, 0)

    pl.semaphore_wait(barrier, len(peers))

    has_rows = lo == tl
    other = 1 - tl
    swaps = []
    for part in range(SWAPS):
        at = pl.ds(part * piece, piece)
        swaps.append(remote(src_ref.at[at], src_in.at[at], s_send.at[part], s_recv.at[part], row_peer(1, 0)))

    def moves_to(block, dual, place, core, send, recv, d_send, d_recv, peer):
        return (
            remote(dual, duals.at[place, core], d_send, d_recv, peer),
            remote(block, blocks.at[place, core], send, recv, peer),
        )

    def f_move(place, own_block):
        block = tgt_ref if own_block else blocks.at[place, tl]
        dual = dual_ref if own_block else duals.at[place, tl]
        return moves_to(
            block, dual, place, tl, f_send.at[place], f_recv.at[place], fd_send.at[place], fd_recv.at[place], col_peer(0, 1)
        )

    def f_arrival(place):
        return moves_to(
            tgt_ref, dual_ref, place, other, f_send.at[place], f_recv.at[place], fd_send.at[place], fd_recv.at[place], col_peer(0, 1)
        )

    sent = [
        moves_to(
            tgt_ref, dual_ref, hi, tl, z_send.at[k], z_recv.at[hi], zd_send.at[k], zd_recv.at[hi], z_peer(ordered[k])
        )
        for k in range(n_hi - 1)
    ]
    sent.append(f_move(hi, True))
    for group in sent[-1:] + sent[:-1]:
        for copy in group:
            copy.start()

    @pl.when(has_rows)
    def _():
        for copy in swaps:
            copy.start()

    blocks[hi, tl] = tgt_ref[...]
    duals[hi, tl] = dual_ref[...]

    def set_right(h, c):
        right[...] = extended(blocks[h, c], 2.0 * SCALE, False)

    def use_block(h, c, first, start, count):
        pots_here = SCALE * duals[h, c]
        chunk = min(DOT_ROWS, count)

        def step(index, carry):
            at = pl.ds(pl.multiple_of(start + index * chunk, chunk), chunk)
            tile = lax.dot_general(
                left[at, :], right[...], (((1,), (1,)), ((), ())), preferred_element_type=jnp.float32
            )
            cost[h, c, at, :] = tile
            scores = [
                tile[:, k : k + LANES] + pots_here[:, k : k + LANES] for k in range(0, own, LANES)
            ]
            high = functools.reduce(jnp.maximum, scores)
            if not first:
                before = top[at, :]
                high = jnp.maximum(high, before)
            total = sum(jnp.exp2(score - high) for score in scores)
            if not first:
                total = total + acc[at, :] * jnp.exp2(before - high)
            top[at, :] = high
            acc[at, :] = total
            return carry

        lax.fori_loop(0, count // chunk, step, 0)

    set_right(hi, tl)
    for part in range(SWAPS):

        @pl.when(has_rows)
        def _(part=part):
            fill_left(src_ref, part)

        @pl.when(jnp.logical_not(has_rows))
        def _(part=part):
            swaps[part].wait_recv()
            fill_left(src_in, part)

        use_block(hi, tl, True, part * piece, piece)
    for copy in f_arrival(hi):
        copy.wait_recv()
    set_right(hi, other)
    use_block(hi, other, False, 0, rows)

    for k in range(n_hi - 1):
        place = ordered[k]
        for copy in moves_to(
            tgt_ref, dual_ref, place, tl, z_send.at[k], z_recv.at[place], zd_send.at[k], zd_recv.at[place], z_peer(place)
        ):
            copy.wait_recv()
        sent.append(f_move(place, False))
        for copy in sent[-1]:
            copy.start()
        set_right(place, tl)
        use_block(place, tl, False, 0, rows)
        for copy in f_arrival(place):
            copy.wait_recv()
        set_right(place, other)
        use_block(place, other, False, 0, rows)

    def row_pass():
        def step(index, carry):
            at = pl.ds(pl.multiple_of(index * 8, 8), 8)
            scores = [
                cost[h, c, at, k : k + LANES] + pots[h : h + 1, c * own + k : c * own + k + LANES]
                for h in range(n_hi)
                for c in range(2)
                for k in range(0, own, LANES)
            ]
            high = functools.reduce(jnp.maximum, scores)
            top[at, :] = high
            acc[at, :] = sum(jnp.exp2(score - high) for score in scores)
            return carry

        lax.fori_loop(0, rows // 8, step, 0, unroll=2)

    def col_pass(h):
        groups = COLS_CHUNK_ROWS // 8

        def step(index, carry):
            high, total = carry
            at = pl.ds(pl.multiple_of(index * COLS_CHUNK_ROWS, COLS_CHUNK_ROWS), COLS_CHUNK_ROWS)
            offs = shift[at, :]
            new_high, new_total = [], []
            tile = jnp.concatenate([cost[h, 0, at, :], cost[h, 1, at, :]], axis=1)
            for k in range(pair // LANES):
                scores = tile[:, k * LANES : (k + 1) * LANES] + offs
                parts = [scores[g * 8 : (g + 1) * 8] for g in range(groups)]
                best = jnp.maximum(high[k], functools.reduce(jnp.maximum, parts))
                part = sum(jnp.exp2(value - best) for value in parts)
                new_total.append(total[k] * jnp.exp2(high[k] - best) + part)
                new_high.append(best)
            return tuple(new_high), tuple(new_total)

        lowest = tuple(jnp.full((8, LANES), -1e38, jnp.float32) for _ in range(pair // LANES))
        zero = tuple(jnp.zeros((8, LANES), jnp.float32) for _ in range(pair // LANES))
        high, total = lax.fori_loop(0, rows // COLS_CHUNK_ROWS, step, (lowest, zero), unroll=2)
        high, total = jnp.concatenate(high, axis=1), jnp.concatenate(total, axis=1)
        best = jnp.max(high, axis=0, keepdims=True)
        return best + log2_of(jnp.sum(total * jnp.exp2(high - best), axis=0, keepdims=True))

    def joined(values):
        best = functools.reduce(jnp.maximum, values)
        return best + log2_of(sum(jnp.exp2(value - best) for value in values))

    pending = []
    for turn in range(ITERS):
        last = turn == ITERS - 1
        if turn:
            row_pass()
        for k in range(rows // LANES):
            high = top[k * LANES : (k + 1) * LANES, :].T
            total = acc[k * LANES : (k + 1) * LANES, :].T
            best = jnp.max(high, axis=0, keepdims=True)
            total = jnp.sum(total * jnp.exp2(high - best), axis=0, keepdims=True)
            row_buf[turn, my_row, k : k + 1, :] = best + log2_of(total)
        copies = []
        for index, move in enumerate(row_moves):
            mine = row_buf.at[turn, my_row]
            copies.append(remote(mine, mine, r_send.at[turn, index], r_recv.at[turn, index], row_peer(*move)))
            copies[-1].start()
        for copy in copies:
            copy.wait_recv()
        pending += copies
        offs = -math.log2(n_dst) - joined([row_buf[turn, g] for g in range(2 * n_th)])
        if last:
            out_mine[...] = offs
            hand = remote(out_mine, out_buf, o_sem.at[0], o_sem.at[1], col_peer(0, 1))

            @pl.when(has_rows)
            def _():
                hand.start()

        for k in range(rows // LANES):
            spread = jnp.broadcast_to(offs[k : k + 1, :], (LANES, LANES))
            shift[k * LANES : (k + 1) * LANES, :] = spread.T
        if not last:
            for h in range(n_hi):
                col_buf[turn, my_col, h : h + 1, :] = col_pass(h)
            copies = []
            for index, move in enumerate(col_moves):
                mine = col_buf.at[turn, my_col]
                copies.append(remote(mine, mine, c_send.at[turn, index], c_recv.at[turn, index], col_peer(*move)))
                copies[-1].start()
            for copy in copies:
                copy.wait_recv()
            pending += copies
            pots[...] = -math.log2(n_src) - joined([col_buf[turn, g] for g in range(2 * n_hi)])
        else:
            for h in range(n_hi):
                value = col_pass(h)
                for c in range(2):
                    fin_mine[h, c] = value[:, c * own : (c + 1) * own]
            copies = []
            for index, (dh, dl) in enumerate(col_moves):
                mine = fin_mine.at[lax.rem(hi + dh, n_hi), lax.rem(tl + dl, 2)]
                copies.append(
                    remote(mine, fin_buf.at[my_col], c_send.at[turn, index], c_recv.at[turn, index], col_peer(dh, dl))
                )
                copies[-1].start()
            fin_buf[my_col] = fin_mine[hi, tl]
            for copy in copies:
                copy.wait_recv()
            pending += copies
            value = -math.log2(n_src) - joined([fin_buf[g] for g in range(2 * n_hi)])
            tgt_out[...] = value

    @pl.when(has_rows)
    def _():
        src_out[...] = out_mine[...]
        hand.wait_send()
        for copy in swaps:
            copy.wait_send()

    @pl.when(jnp.logical_not(has_rows))
    def _():
        hand.wait_recv()
        src_out[...] = out_buf[...]

    for group in sent:
        for copy in group:
            copy.wait_send()
    for copy in pending:
        copy.wait_send()


def body(sources, targets, duals_init, n_hi, n_th):
    rows, width = sources.shape
    own = targets.shape[0]
    pair = 2 * own
    vmem = pl.BlockSpec(memory_space=pltpu.VMEM)
    dma = pltpu.SemaphoreType.DMA
    f32 = jnp.float32
    source_pots, target_pots = pl.pallas_call(
        functools.partial(kernel, n_hi, n_th),
        out_shape=(
            jax.ShapeDtypeStruct((rows // LANES, LANES), f32),
            jax.ShapeDtypeStruct((1, own), f32),
        ),
        in_specs=[vmem] * 3,
        out_specs=(vmem, vmem),
        scratch_shapes=[
            pltpu.VMEM((rows, width), f32),
            pltpu.VMEM((rows, 4 * width), jnp.bfloat16),
            pltpu.VMEM((own, 4 * width), jnp.bfloat16),
            pltpu.VMEM((n_hi, 2, rows, own), f32),
            pltpu.VMEM((n_hi, 2, own, width), f32),
            pltpu.VMEM((n_hi, 2, 1, own), f32),
            pltpu.VMEM((rows, LANES), f32),
            pltpu.VMEM((rows, LANES), f32),
            pltpu.VMEM((rows, LANES), f32),
            pltpu.VMEM((n_hi, pair), f32),
            pltpu.VMEM((ITERS, 2 * n_th, rows // LANES, LANES), f32),
            pltpu.VMEM((ITERS, 2 * n_hi, n_hi, pair), f32),
            pltpu.VMEM((n_hi, 2, 1, own), f32),
            pltpu.VMEM((2 * n_hi, 1, own), f32),
            pltpu.VMEM((rows // LANES, LANES), f32),
            pltpu.VMEM((rows // LANES, LANES), f32),
            dma((SWAPS,)), dma((SWAPS,)),
            dma((n_hi,)), dma((n_hi,)), dma((n_hi,)), dma((n_hi,)),
            dma((n_hi,)), dma((n_hi,)), dma((n_hi,)), dma((n_hi,)),
            dma((ITERS, 2 * n_th)), dma((ITERS, 2 * n_th)),
            dma((ITERS, 2 * n_hi)), dma((ITERS, 2 * n_hi)),
            dma((2,)),
        ],
        compiler_params=pltpu.CompilerParams(
            collective_id=0, has_side_effects=True, vmem_limit_bytes=60 * 1024 * 1024
        ),
    )(sources, targets, duals_init.reshape(1, own))
    return source_pots.reshape(rows) * (1.0 / SCALE), target_pots.reshape(own) * (1.0 / SCALE)


def solution(mesh):
    n_hi, n_th = mesh.shape["blk"] // 2, mesh.shape["tgt"] // 2
    return jax.shard_map(
        functools.partial(body, n_hi=n_hi, n_th=n_th),
        mesh=mesh,
        in_specs=(P("blk", None), P(("blk", "tgt"), None), P(("blk", "tgt"))),
        out_specs=(P("blk"), P(("blk", "tgt"))),
        check_vma=False,
    )
```

```python
import functools
import math

import jax
import jax.numpy as jnp
from jax import lax
from jax.experimental import pallas as pl
from jax.experimental.pallas import tpu as pltpu
from jax.sharding import PartitionSpec as P

ITERS = 2
EPS = 0.05
LOG2E = math.log2(math.e)
SCALE = LOG2E / EPS
MESH = pl.DeviceIdType.MESH
LANES = 128
COLS_CHUNK_ROWS = 128
DOT_ROWS = 512
SWAPS = 4


def log2_of(value):
    return jnp.log(value) * LOG2E


def pieces_of(value, count):
    parts = []
    for _ in range(count):
        part = value.astype(jnp.bfloat16)
        parts.append(part)
        value = value - part.astype(jnp.float32)
    return parts


def extended(points, scale, norm_first):
    norm = -SCALE * jnp.sum(points * points, axis=1, keepdims=True)
    hi, lo = pieces_of(points * scale, 2)
    first, second, third = (part.astype(jnp.float32) for part in pieces_of(norm, 3))
    lane = lax.broadcasted_iota(jnp.int32, points.shape, 1)
    base = 0 if norm_first else 3
    ones = 3 - base
    extra = jnp.where((lane >= ones) & (lane < ones + 3), 1.0, 0.0)
    extra = jnp.where(lane == base, first, extra)
    extra = jnp.where(lane == base + 1, second, extra)
    extra = jnp.where(lane == base + 2, third, extra)
    middle = (lo, hi) if norm_first else (hi, lo)
    return jnp.concatenate([hi, middle[0], middle[1], extra.astype(jnp.bfloat16)], axis=1)


def kernel(
    n_hi, n_th, src_ref, tgt_ref, dual_ref, src_out, tgt_out,
    src_in, left, right, cost, blocks, duals, top, acc, shift, pots, row_buf, col_buf, fin_mine, fin_buf, out_mine, out_buf,
    s_send, s_recv, z_send, z_recv, zd_send, zd_recv, f_send, f_recv, fd_send, fd_recv, r_send, r_recv, c_send, c_recv, o_sem,
):
    rows, width = src_ref.shape
    own = tgt_ref.shape[0]
    pair = 2 * own
    n_src = rows * n_hi * 2
    n_dst = own * n_hi * 2 * n_th * 2
    b, t = lax.axis_index("blk"), lax.axis_index("tgt")
    hi, lo = lax.div(b, 2), lax.rem(b, 2)
    th, tl = lax.div(t, 2), lax.rem(t, 2)

    def col_peer(dh, dl):
        return (lax.rem(hi + dh, n_hi) * 2 + lo, th * 2 + lax.rem(tl + dl, 2))

    def row_peer(dlo, dth):
        return (hi * 2 + lax.rem(lo + dlo, 2), lax.rem(th + dth, n_th) * 2 + tl)

    col_moves = [(dh, dl) for dh in range(n_hi) for dl in range(2) if dh or dl]
    row_moves = [(dlo, dth) for dlo in range(2) for dth in range(n_th) if dlo or dth]
    my_col = hi * 2 + tl
    my_row = lo * n_th + th

    def remote(src, dst, send, recv, peer):
        return pltpu.make_async_remote_copy(
            src_ref=src, dst_ref=dst, send_sem=send, recv_sem=recv, device_id=peer, device_id_type=MESH
        )

    barrier = pltpu.get_barrier_semaphore()
    peers = [col_peer(*move) for move in col_moves] + [row_peer(*move) for move in row_moves]
    for peer in peers:
        pl.semaphore_signal(barrier, inc=1, device_id=peer, device_id_type=MESH)

    ordered = [jnp.int32(0)] * (n_hi - 1)
    found = jnp.int32(0)
    for distance in range(1, n_hi):
        for place in (hi - distance, hi + distance):
            valid = jnp.where((place >= 0) & (place < n_hi), 1, 0)
            for k in range(n_hi - 1):
                ordered[k] = ordered[k] + jnp.where(found == k, 1, 0) * valid * place
            found = found + valid

    def z_peer(place):
        return (place * 2 + lo, t)

    piece = rows // SWAPS

    def fill_left(ref, part):
        def step(index, carry):
            at = pl.ds(pl.multiple_of(part * piece + index * LANES, LANES), LANES)
            left[at, :] = extended(ref[at, :], 1.0, True)
            return carry

        lax.fori_loop(0, piece // LANES, step, 0)

    def set_right(h, c):
        right[...] = extended(blocks[h, c], 2.0 * SCALE, False)

    has_rows = lo == tl
    blocks[hi, tl] = tgt_ref[...]
    duals[hi, tl] = dual_ref[...]
    set_right(hi, tl)

    @pl.when(has_rows)
    def _():
        for part in range(SWAPS):
            fill_left(src_ref, part)

    pl.semaphore_wait(barrier, len(peers))

    other = 1 - tl
    swaps = []
    for part in range(SWAPS):
        at = pl.ds(part * piece, piece)
        swaps.append(remote(src_ref.at[at], src_in.at[at], s_send.at[part], s_recv.at[part], row_peer(1, 0)))

    def moves_to(block, dual, place, core, send, recv, d_send, d_recv, peer):
        return (
            remote(dual, duals.at[place, core], d_send, d_recv, peer),
            remote(block, blocks.at[place, core], send, recv, peer),
        )

    def f_move(place, own_block):
        block = tgt_ref if own_block else blocks.at[place, tl]
        dual = dual_ref if own_block else duals.at[place, tl]
        return moves_to(
            block, dual, place, tl, f_send.at[place], f_recv.at[place], fd_send.at[place], fd_recv.at[place], col_peer(0, 1)
        )

    def f_arrival(place):
        return moves_to(
            tgt_ref, dual_ref, place, other, f_send.at[place], f_recv.at[place], fd_send.at[place], fd_recv.at[place], col_peer(0, 1)
        )

    sent = [
        moves_to(
            tgt_ref, dual_ref, hi, tl, z_send.at[k], z_recv.at[hi], zd_send.at[k], zd_recv.at[hi], z_peer(ordered[k])
        )
        for k in range(n_hi - 1)
    ]
    sent.append(f_move(hi, True))
    for group in sent[-1:] + sent[:-1]:
        for copy in group:
            copy.start()

    @pl.when(has_rows)
    def _():
        for copy in swaps:
            copy.start()

    def use_block(h, c, first, start, count):
        pots_here = SCALE * duals[h, c]
        chunk = min(DOT_ROWS, count)

        def step(index, carry):
            at = pl.ds(pl.multiple_of(start + index * chunk, chunk), chunk)
            tile = lax.dot_general(
                left[at, :], right[...], (((1,), (1,)), ((), ())), preferred_element_type=jnp.float32
            )
            cost[h, c, at, :] = tile
            scores = [
                tile[:, k : k + LANES] + pots_here[:, k : k + LANES] for k in range(0, own, LANES)
            ]
            high = functools.reduce(jnp.maximum, scores)
            if not first:
                before = top[at, :]
                high = jnp.maximum(high, before)
            total = sum(jnp.exp2(score - high) for score in scores)
            if not first:
                total = total + acc[at, :] * jnp.exp2(before - high)
            top[at, :] = high
            acc[at, :] = total
            return carry

        lax.fori_loop(0, count // chunk, step, 0)

    for part in range(SWAPS):

        @pl.when(jnp.logical_not(has_rows))
        def _(part=part):
            swaps[part].wait_recv()
            fill_left(src_in, part)

        use_block(hi, tl, True, part * piece, piece)
    for copy in f_arrival(hi):
        copy.wait_recv()
    set_right(hi, other)
    use_block(hi, other, False, 0, rows)

    for k in range(n_hi - 1):
        place = ordered[k]
        for copy in moves_to(
            tgt_ref, dual_ref, place, tl, z_send.at[k], z_recv.at[place], zd_send.at[k], zd_recv.at[place], z_peer(place)
        ):
            copy.wait_recv()
        sent.append(f_move(place, False))
        for copy in sent[-1]:
            copy.start()
        set_right(place, tl)
        use_block(place, tl, False, 0, rows)
        for copy in f_arrival(place):
            copy.wait_recv()
        set_right(place, other)
        use_block(place, other, False, 0, rows)

    def row_pass():
        def step(index, carry):
            at = pl.ds(pl.multiple_of(index * 8, 8), 8)
            scores = [
                cost[h, c, at, k : k + LANES] + pots[h : h + 1, c * own + k : c * own + k + LANES]
                for h in range(n_hi)
                for c in range(2)
                for k in range(0, own, LANES)
            ]
            high = functools.reduce(jnp.maximum, scores)
            top[at, :] = high
            acc[at, :] = sum(jnp.exp2(score - high) for score in scores)
            return carry

        lax.fori_loop(0, rows // 8, step, 0, unroll=16)

    def col_pass(h):
        groups = COLS_CHUNK_ROWS // 8

        def step(index, carry):
            high, total = carry
            at = pl.ds(pl.multiple_of(index * COLS_CHUNK_ROWS, COLS_CHUNK_ROWS), COLS_CHUNK_ROWS)
            offs = shift[at, :]
            new_high, new_total = [], []
            tile = jnp.concatenate([cost[h, 0, at, :], cost[h, 1, at, :]], axis=1)
            for k in range(pair // LANES):
                scores = tile[:, k * LANES : (k + 1) * LANES] + offs
                parts = [scores[g * 8 : (g + 1) * 8] for g in range(groups)]
                best = jnp.maximum(high[k], functools.reduce(jnp.maximum, parts))
                part = sum(jnp.exp2(value - best) for value in parts)
                new_total.append(total[k] * jnp.exp2(high[k] - best) + part)
                new_high.append(best)
            return tuple(new_high), tuple(new_total)

        lowest = tuple(jnp.full((8, LANES), -1e38, jnp.float32) for _ in range(pair // LANES))
        zero = tuple(jnp.zeros((8, LANES), jnp.float32) for _ in range(pair // LANES))
        high, total = lax.fori_loop(0, rows // COLS_CHUNK_ROWS, step, (lowest, zero), unroll=4)
        high, total = jnp.concatenate(high, axis=1), jnp.concatenate(total, axis=1)
        best = jnp.max(high, axis=0, keepdims=True)
        return best + log2_of(jnp.sum(total * jnp.exp2(high - best), axis=0, keepdims=True))

    def joined(values):
        best = functools.reduce(jnp.maximum, values)
        return best + log2_of(sum(jnp.exp2(value - best) for value in values))

    pending = []
    for turn in range(ITERS):
        last = turn == ITERS - 1
        if turn:
            row_pass()
        for k in range(rows // LANES):
            high = top[k * LANES : (k + 1) * LANES, :].T
            total = acc[k * LANES : (k + 1) * LANES, :].T
            best = jnp.max(high, axis=0, keepdims=True)
            total = jnp.sum(total * jnp.exp2(high - best), axis=0, keepdims=True)
            row_buf[turn, my_row, k : k + 1, :] = best + log2_of(total)
        copies = []
        for index, move in enumerate(row_moves):
            mine = row_buf.at[turn, my_row]
            copies.append(remote(mine, mine, r_send.at[turn, index], r_recv.at[turn, index], row_peer(*move)))
            copies[-1].start()
        for copy in copies:
            copy.wait_recv()
        pending += copies
        offs = -math.log2(n_dst) - joined([row_buf[turn, g] for g in range(2 * n_th)])
        if last:
            out_mine[...] = offs
            hand = remote(out_mine, out_buf, o_sem.at[0], o_sem.at[1], col_peer(0, 1))

            @pl.when(has_rows)
            def _():
                hand.start()

        for k in range(rows // LANES):
            spread = jnp.broadcast_to(offs[k : k + 1, :], (LANES, LANES))
            shift[k * LANES : (k + 1) * LANES, :] = spread.T
        if not last:
            for h in range(n_hi):
                col_buf[turn, my_col, h : h + 1, :] = col_pass(h)
            copies = []
            for index, move in enumerate(col_moves):
                mine = col_buf.at[turn, my_col]
                copies.append(remote(mine, mine, c_send.at[turn, index], c_recv.at[turn, index], col_peer(*move)))
                copies[-1].start()
            for copy in copies:
                copy.wait_recv()
            pending += copies
            pots[...] = -math.log2(n_src) - joined([col_buf[turn, g] for g in range(2 * n_hi)])
        else:
            for h in range(n_hi):
                value = col_pass(h)
                for c in range(2):
                    fin_mine[h, c] = value[:, c * own : (c + 1) * own]
            copies = []
            for index, (dh, dl) in enumerate(col_moves):
                mine = fin_mine.at[lax.rem(hi + dh, n_hi), lax.rem(tl + dl, 2)]
                copies.append(
                    remote(mine, fin_buf.at[my_col], c_send.at[turn, index], c_recv.at[turn, index], col_peer(dh, dl))
                )
                copies[-1].start()
            fin_buf[my_col] = fin_mine[hi, tl]
            for copy in copies:
                copy.wait_recv()
            pending += copies
            value = -math.log2(n_src) - joined([fin_buf[g] for g in range(2 * n_hi)])
            tgt_out[...] = value

    @pl.when(has_rows)
    def _():
        src_out[...] = out_mine[...]
        hand.wait_send()
        for copy in swaps:
            copy.wait_send()

    @pl.when(jnp.logical_not(has_rows))
    def _():
        hand.wait_recv()
        src_out[...] = out_buf[...]

    for group in sent:
        for copy in group:
            copy.wait_send()
    for copy in pending:
        copy.wait_send()


def body(sources, targets, duals_init, n_hi, n_th):
    rows, width = sources.shape
    own = targets.shape[0]
    pair = 2 * own
    vmem = pl.BlockSpec(memory_space=pltpu.VMEM)
    dma = pltpu.SemaphoreType.DMA
    f32 = jnp.float32
    source_pots, target_pots = pl.pallas_call(
        functools.partial(kernel, n_hi, n_th),
        out_shape=(
            jax.ShapeDtypeStruct((rows // LANES, LANES), f32),
            jax.ShapeDtypeStruct((1, own), f32),
        ),
        in_specs=[vmem] * 3,
        out_specs=(vmem, vmem),
        scratch_shapes=[
            pltpu.VMEM((rows, width), f32),
            pltpu.VMEM((rows, 4 * width), jnp.bfloat16),
            pltpu.VMEM((own, 4 * width), jnp.bfloat16),
            pltpu.VMEM((n_hi, 2, rows, own), f32),
            pltpu.VMEM((n_hi, 2, own, width), f32),
            pltpu.VMEM((n_hi, 2, 1, own), f32),
            pltpu.VMEM((rows, LANES), f32),
            pltpu.VMEM((rows, LANES), f32),
            pltpu.VMEM((rows, LANES), f32),
            pltpu.VMEM((n_hi, pair), f32),
            pltpu.VMEM((ITERS, 2 * n_th, rows // LANES, LANES), f32),
            pltpu.VMEM((ITERS, 2 * n_hi, n_hi, pair), f32),
            pltpu.VMEM((n_hi, 2, 1, own), f32),
            pltpu.VMEM((2 * n_hi, 1, own), f32),
            pltpu.VMEM((rows // LANES, LANES), f32),
            pltpu.VMEM((rows // LANES, LANES), f32),
            dma((SWAPS,)), dma((SWAPS,)),
            dma((n_hi,)), dma((n_hi,)), dma((n_hi,)), dma((n_hi,)),
            dma((n_hi,)), dma((n_hi,)), dma((n_hi,)), dma((n_hi,)),
            dma((ITERS, 2 * n_th)), dma((ITERS, 2 * n_th)),
            dma((ITERS, 2 * n_hi)), dma((ITERS, 2 * n_hi)),
            dma((2,)),
        ],
        compiler_params=pltpu.CompilerParams(
            collective_id=0, has_side_effects=True, vmem_limit_bytes=60 * 1024 * 1024
        ),
    )(sources, targets, duals_init.reshape(1, own))
    return source_pots.reshape(rows) * (1.0 / SCALE), target_pots.reshape(own) * (1.0 / SCALE)


def solution(mesh):
    n_hi, n_th = mesh.shape["blk"] // 2, mesh.shape["tgt"] // 2
    return jax.shard_map(
        functools.partial(body, n_hi=n_hi, n_th=n_th),
        mesh=mesh,
        in_specs=(P("blk", None), P(("blk", "tgt"), None), P(("blk", "tgt"))),
        out_specs=(P("blk"), P(("blk", "tgt"))),
        check_vma=False,
    )
```
